256 devices in a mesh: arcs: 16 (over x, y_hi, core), tiles: 16 (over z, y_lo).
Axes of the slice: x: 4, y: 4 (y_hi: 2, y_lo: 2; y = y_hi * 2 + y_lo), z: 8, core: 2. Of those that a mesh axis runs over, the one named last changes fastest.
Arguments:
- design: bfloat16 [24576, 8192], P('arcs', 'tiles'), may hold values from -0.09375 to 0.09375
- observations: float32 [24576], P('arcs'), may hold values from -25 to 25
- solution: float32 [8192], P('tiles'), may hold values from -6 to 6
- arc_ids: int32 [16, 1536], P('arcs'), may hold values from 0 to 3, never falling along the last dimension, each value on 1 to 768 neighbouring positions
- block_live: int32 [16, 12], P('arcs'), may hold values 0 or 1
Outputs:
- normal: float32 [8192, 8192], P('arcs', 'tiles')
- rhs: float32 [8192], P('tiles')
The draws below stay inside these ranges and needn't reach their ends.
Inputs may be any that keep to these rules, and one draw needn't show every extreme that they name: `arc_ids`: the arcs of a group's rows never fall along its rows; an arc holds at most 768 rows and some arc exactly that many.
All inputs are finite; a program needn't handle non-finite values. No bound on the sum of `block_live` on one device may be relied on, other than what follows from the above.
Results may differ from the reference program's by a relative error of at most 0.0018.
Values may be sent and summed in bfloat16 or wider, within the bound.
No kernel may reach another device: no remote copies, remote signals or barrier semaphores. Data moves between devices by JAX's collectives and lax.ppermute only.
A program may use at most 128 MiB of HBM per device.

```python
import math
import jax
import jax.numpy as jnp
import numpy as np
from jax import lax

COEF = 8192
ROWS_DEV = 1536
ARCS_DEV = 4
SEG_MOST = 768
BLOCKS = 12
TOTAL_ROWS = 24576
N_ARCS = 16


def draw_observations(key, part):
    first_key, second_key = jax.random.split(jax.random.fold_in(key, 11))
    position = jnp.arange(TOTAL_ROWS, dtype=jnp.int32)
    denominator = max(TOTAL_ROWS // ROWS_DEV - 1, 1)
    device_frac = (position // ROWS_DEV).astype(jnp.float32) / denominator
    group_scale = jnp.exp(jax.random.uniform(second_key, (TOTAL_ROWS // 64,), minval=-0.5, maxval=0.5))
    local_scale = jnp.repeat(group_scale, 64)
    noise = jnp.clip(jax.random.normal(first_key, (TOTAL_ROWS,)), -5.0, 5.0)
    return (noise * (1.0 + 2.0 * device_frac) * local_scale).astype(jnp.float32)


def set_ends(result, stream_key, low, high):
    index_at = [jax.random.randint(jax.random.fold_in(stream_key, axis), (), 0, length) for axis, length in enumerate(result.shape)]
    longest = result.shape.index(max(result.shape))
    neighbour = index_at[:longest] + [(index_at[longest] + 1) % result.shape[longest]] + index_at[longest + 1:]
    return result.at[tuple(index_at)].set(low).at[tuple(neighbour)].set(high)


def raised(drawn, stream_key, source, target, parts, factor):
    owner, partner = [(jnp.arange(drawn.shape[dim]) // (drawn.shape[dim] // parts)).reshape([-1 if axis == dim else 1 for axis in range(drawn.ndim)]) for dim in (source, target)]
    chosen = jax.random.permutation(stream_key, parts)[partner]
    strong = (owner == chosen) | (owner == (partner + parts // 2) % parts)
    return jnp.where(strong, factor * drawn, drawn)


def shard_levels(own_key, dims, cuts, low, largest):
    def one(dim, blocks):
        steps = jax.random.uniform(jax.random.fold_in(jax.random.fold_in(own_key, 6), dim), (blocks,), jnp.float32, low / len(cuts), largest / len(cuts))
        return jnp.repeat(jnp.exp(steps), dims[dim] // blocks).reshape((-1,) + (1,) * (len(dims) - dim - 1))

    level = one(*cuts[0])
    for cut in cuts[1:]:
        level = level * one(*cut)
    return level


def split_up(number_of, total, bound, skew):
    portions = [(1 << 20) // math.isqrt(standing ** skew) + 1 for standing in range(2, number_of + 1)]
    spare, holding = total - bound - (number_of - 1), [1] * (number_of - 1)
    while spare > 0:
        free = [i for i in range(number_of - 1) if holding[i] < bound]
        whole, budget = sum([portions[i] for i in free]), spare
        for i in free:
            more = min(bound - holding[i], max(1, budget * portions[i] // whole), spare)
            holding[i] = holding[i] + more
            spare = spare - more
    return np.array([bound] + holding)


def uneven(own_key, amount, total, most, skew):
    if amount == 2:
        one = jax.random.randint(own_key, (), max(1, total - most), min(most, total - 1) + 1)
        return jnp.stack([one, total - one])
    tallies = jnp.asarray(split_up(amount, total, most, skew), jnp.int32)
    twos = (amount - 1) // 2
    giver, receiver = tallies[1:1 + 2 * twos:2], tallies[2:2 + 2 * twos:2]
    margin = jnp.minimum(giver - 1, most - receiver)
    moved = jax.random.randint(jax.random.fold_in(own_key, 1), (twos,), 0, 1 << 20) % (margin + 1)
    tallies = tallies.at[1:1 + 2 * twos:2].set(giver - moved).at[2:2 + 2 * twos:2].set(receiver + moved)
    return tallies[jax.random.permutation(jax.random.fold_in(own_key, 2), amount)]


def gaussian(rng, shape, width, reach, cuts=(), kind=jnp.bfloat16):
    values = jax.random.normal(rng, shape, jnp.float32) * width
    if len(cuts) > 0:
        values = shard_levels(rng, shape, cuts, -0.22, 0.18) * values
    return jnp.clip(values, min=-reach, max=reach).astype(kind)


def gaussian_with(own_key, shape, width, limit, pieces, heavy, kind=jnp.bfloat16):
    entries = width * jax.random.normal(own_key, shape, jnp.float32)
    if pieces:
        entries = entries * shard_levels(own_key, shape, pieces, -0.22, 0.18)
    return jnp.clip(raised(entries, jax.random.fold_in(own_key, 3), *heavy), -limit, limit).astype(kind)


def setup_inputs(seed: int = 0) -> dict:
    key_of = jax.random.split(jax.random.key(seed), 6)
    design = gaussian_with(key_of[0], (TOTAL_ROWS, COEF), COEF ** -0.5, 0.09375, ((0, 16), (1, 16)), (0, 1, 16, 2.0))
    observations = draw_observations(jax.random.fold_in(key_of[5], 71), 0)
    solution = gaussian(key_of[2], (COEF,), 1.0, 6.0, ((0, 16),), jnp.float32)
    arc_ids = jax.vmap(lambda own: jnp.searchsorted(jnp.cumsum(uneven(own, ARCS_DEV, ROWS_DEV, SEG_MOST, 2)), jnp.arange(ROWS_DEV), side="right"))(jax.random.split(key_of[3], N_ARCS)).reshape((N_ARCS, ROWS_DEV)).astype(jnp.int32)
    block_live = set_ends((jax.random.randint(key_of[4], (N_ARCS, BLOCKS), 0, 4) < 3).astype(jnp.int32), jax.random.fold_in(key_of[4], 1), 0, 1)
    return {"design": design, "observations": observations, "solution": solution, "arc_ids": arc_ids, "block_live": block_live}


prior_rows = 4.0


def reference(design, observations, solution, arc_ids, block_live):
    groups = arc_ids.shape[0]
    per_group = arc_ids.shape[1]
    row_count = groups * per_group
    live_row = jnp.broadcast_to(block_live[:, :, None], (groups, block_live.shape[1], 128)).reshape(row_count).astype(jnp.float32)
    design_wide = design.astype(jnp.float32)
    predicted = jnp.dot(design_wide, solution, precision=lax.Precision.HIGHEST)
    residual = observations - predicted
    squares = (live_row * residual * residual).reshape(groups, per_group)
    live_group = live_row.reshape(groups, per_group)
    arc_match = (arc_ids[:, None, :] == jnp.arange(ARCS_DEV, dtype=jnp.int32)[None, :, None]).astype(jnp.float32)
    arc_squares = jnp.sum(arc_match * squares[:, None, :], axis=2)
    arc_counts = jnp.sum(arc_match * live_group[:, None, :], axis=2)
    variance_all = (jnp.sum(arc_squares) + 1.0) / (jnp.sum(arc_counts) + 1.0)
    arc_weight = variance_all / ((arc_squares + prior_rows * variance_all) / (arc_counts + prior_rows))
    row_weight = live_row * jnp.sum(arc_match * arc_weight[:, :, None], axis=1).reshape(row_count)
    weighted = (row_weight[:, None] * design_wide).astype(jnp.bfloat16)
    normal = jnp.dot(design_wide.T, weighted.astype(jnp.float32), precision=lax.Precision.HIGHEST)
    rhs = jnp.dot(design_wide.T, row_weight * residual, precision=lax.Precision.HIGHEST)
    return normal, rhs
```

```python
import jax
import jax.numpy as jnp
from jax import lax
from jax.sharding import Mesh
from jax.sharding import PartitionSpec as P

ARCS_DEV = 4
ARCS = ("x", "yh", "core")
TILES = ("z", "yl")
CHUNKS = 4
prior_rows = 4.0
f32, bf16 = jnp.float32, jnp.bfloat16


def of_everyone(array, axis):
    count = lax.axis_size(axis)
    sent = jnp.broadcast_to(array[None], (count, *array.shape))
    return lax.all_to_all(sent, axis, 0, 0, tiled=True).sum(axis=0)


def local(design, observations, solution, arc_ids, block_live):
    rows, cols = design.shape
    width = cols // CHUNKS
    core, yl = lax.axis_index("core"), lax.axis_index("yl")
    gathered = [
        lax.all_gather(design[:, j * width : (j + 1) * width], "z", axis=0)
        for j in range(CHUNKS)
    ]
    other = lax.ppermute(design, "yl", [(0, 1), (1, 0)])
    partial_value = jnp.dot(design.astype(f32), solution, precision=lax.Precision.HIGHEST)
    predicted = of_everyone(partial_value, TILES)
    residual = observations - predicted
    live_row = (
        jnp.broadcast_to(block_live[0][:, None], (block_live.shape[1], 128))
        .reshape(rows)
        .astype(f32)
    )
    arc_match = (arc_ids[0][None, :] == jnp.arange(ARCS_DEV, dtype=jnp.int32)[:, None]).astype(f32)
    squares = live_row * residual * residual
    arc_squares = jnp.sum(arc_match * squares[None, :], axis=1)
    arc_counts = jnp.sum(arc_match * live_row[None, :], axis=1)
    totals = of_everyone(jnp.stack([jnp.sum(arc_squares), jnp.sum(arc_counts)]), ARCS)
    variance_all = (totals[0] + 1.0) / (totals[1] + 1.0)
    arc_weight = variance_all / (
        (arc_squares + prior_rows * variance_all) / (arc_counts + prior_rows)
    )
    row_weight = live_row * jnp.sum(arc_match * arc_weight[:, None], axis=0)
    rhs_part = lax.dot_general(
        design.astype(f32),
        row_weight * residual,
        (((0,), (0,)), ((), ())),
        precision=lax.Precision.HIGHEST,
    )
    mine = jnp.where(core == yl, design, other)
    theirs = jnp.where(core == yl, other, design)
    weighted_mine = (row_weight[:, None] * mine).astype(bf16)
    weighted_theirs = (row_weight[:, None] * theirs).astype(bf16)

    def product(left, right):
        return lax.dot_general(left, right, (((1,), (0,)), ((), ())), preferred_element_type=f32)

    rank = lax.axis_index(("x", "yh"))
    done = []
    for j in range(CHUNKS):
        sent = product(gathered[j], weighted_theirs)
        kept = product(gathered[j], weighted_mine)
        pair = kept + lax.ppermute(sent, "core", [(0, 1), (1, 0)])
        got = lax.all_to_all(pair.astype(bf16), ("x", "yh"), 0, 0, tiled=True)
        done.append(jnp.sum(got.astype(f32), axis=0))
    block = jnp.concatenate(done, axis=0)
    swap = [(0, 0), (1, 2), (2, 1), (3, 3)]
    normal = lax.ppermute(block, ("core", "yl"), swap)
    rhs = of_everyone(rhs_part, ARCS)
    return normal, rhs


def solution(mesh):
    finer = Mesh(mesh.devices.reshape(4, 2, 2, 8, 2), ARCS + TILES)
    return jax.shard_map(
        local,
        mesh=finer,
        in_specs=(P(ARCS, TILES), P(ARCS), P(TILES), P(ARCS, None), P(ARCS, None)),
        out_specs=(P(ARCS, TILES), P(TILES)),
        check_vma=False,
    )
```

```python
import jax
import jax.numpy as jnp
from jax import lax
from jax.sharding import Mesh
from jax.sharding import PartitionSpec as P

ARCS_DEV = 4
ARCS = ("x", "yh", "core")
TILES = ("z", "yl")
WIDTHS = (256, 128, 128)
PAIR = [(0, 1), (1, 0)]
prior_rows = 4.0
f32, bf16 = jnp.float32, jnp.bfloat16


def after(array, *first):
    return lax.optimization_barrier((array, *first))[0]


def of_everyone(array, axis):
    count = lax.axis_size(axis)
    sent = jnp.broadcast_to(array[None], (count, *array.shape))
    return lax.all_to_all(sent, axis, 0, 0, tiled=True).sum(axis=0)


def local(design, observations, solution, arc_ids, block_live):
    rows, _ = design.shape
    core, yl = lax.axis_index("core"), lax.axis_index("yl")
    gathered, begin = [], 0
    for width in WIDTHS:
        gathered.append(lax.all_gather(design[:, begin : begin + width], "z", axis=0))
        begin += width
    partial_value = jnp.dot(design.astype(f32), solution, precision=lax.Precision.HIGHEST)
    from_pair = lax.ppermute(partial_value, "yl", PAIR)
    other = lax.ppermute(after(design, from_pair), "yl", PAIR)
    predicted = of_everyone(partial_value + from_pair, "z")
    residual = observations - predicted
    live_row = (
        jnp.broadcast_to(block_live[0][:, None], (block_live.shape[1], 128))
        .reshape(rows)
        .astype(f32)
    )
    arc_match = (arc_ids[0][None, :] == jnp.arange(ARCS_DEV, dtype=jnp.int32)[:, None]).astype(f32)
    squares = live_row * residual * residual
    arc_squares = jnp.sum(arc_match * squares[None, :], axis=1)
    arc_counts = jnp.sum(arc_match * live_row[None, :], axis=1)
    totals = of_everyone(jnp.stack([jnp.sum(arc_squares), jnp.sum(arc_counts)]), ARCS)
    variance_all = (totals[0] + 1.0) / (totals[1] + 1.0)
    arc_weight = variance_all / (
        (arc_squares + prior_rows * variance_all) / (arc_counts + prior_rows)
    )
    row_weight = live_row * jnp.sum(arc_match * arc_weight[:, None], axis=0)
    rhs_part = lax.dot_general(
        design.astype(f32),
        row_weight * residual,
        (((0,), (0,)), ((), ())),
        precision=lax.Precision.HIGHEST,
    )
    rhs_pair = rhs_part + lax.ppermute(rhs_part, "core", PAIR)
    rhs = of_everyone(rhs_pair, ("x", "yh"))
    weighted_own = (row_weight[:, None] * design).astype(bf16)
    weighted_other = (row_weight[:, None] * other).astype(bf16)
    mine = jnp.where(core == yl, weighted_own, weighted_other)
    theirs = jnp.where(core == yl, weighted_other, weighted_own)

    def product(left, right):
        return lax.dot_general(left, right, (((1,), (0,)), ((), ())), preferred_element_type=f32)

    done, swap = [], [(0, 0), (1, 2), (2, 1), (3, 3)]
    for j, left in enumerate(gathered):
        sent = product(left, theirs if j else after(theirs, rhs))
        from_core = lax.ppermute(sent, "core", PAIR)
        pair = (product(left, mine) + from_core).astype(bf16)
        got = lax.all_to_all(pair, ("x", "yh"), 0, 0, tiled=True)
        block = jnp.sum(got.astype(f32), axis=0)
        done.append(lax.ppermute(block, ("core", "yl"), swap))
    return jnp.concatenate(done, axis=0), rhs


def solution(mesh):
    finer = Mesh(mesh.devices.reshape(4, 2, 2, 8, 2), ARCS + TILES)
    return jax.shard_map(
        local,
        mesh=finer,
        in_specs=(P(ARCS, TILES), P(ARCS), P(TILES), P(ARCS, None), P(ARCS, None)),
        out_specs=(P(ARCS, TILES), P(TILES)),
        check_vma=False,
    )
```

```python
import jax
import jax.numpy as jnp
from jax import lax
from jax.experimental import pallas as pl
from jax.experimental.pallas import tpu as pltpu
from jax.sharding import Mesh
from jax.sharding import PartitionSpec as P

ARCS_DEV = 4
ARCS = ("x", "yh", "core")
TILES = ("z", "yl")
FIRST, WIDTH = 256, 128
prior_rows = 4.0
f32, bf16 = jnp.float32, jnp.bfloat16
PAIR = [(0, 1), (1, 0)]


def after(array, *first):
    return lax.optimization_barrier((array, *first))[0]


def of_everyone(array, axis):
    count = lax.axis_size(axis)
    sent = jnp.broadcast_to(array[None], (count, *array.shape))
    return lax.all_to_all(sent, axis, 0, 0, tiled=True).sum(axis=0)


def product(place, blocks, right, added=None):
    count, (rows, width), cols = len(blocks), blocks[0].shape, right.shape[1]
    dtype = f32 if added is None else bf16

    def kernel(place_ref, *refs):
        right_ref, out_ref = refs[count], refs[-1]
        for i in range(count):
            part = lax.dot_general(
                refs[i][...],
                right_ref[...],
                (((0,), (0,)), ((), ())),
                preferred_element_type=f32,
            )
            at = place_ref[i]
            if added is not None:
                part = part + refs[count + 1][at]
            out_ref[at] = part.astype(dtype)

    extra = [] if added is None else [added]
    vmem = pl.BlockSpec(memory_space=pltpu.VMEM)
    return pl.pallas_call(
        kernel,
        out_shape=jax.ShapeDtypeStruct((count, width, cols), dtype),
        in_specs=[pl.BlockSpec(memory_space=pltpu.SMEM)] + [vmem] * (count + 1 + len(extra)),
        out_specs=vmem,
        cost_estimate=pl.CostEstimate(
            flops=2 * count * rows * width * cols,
            bytes_accessed=2 * count * rows * width + 2 * rows * cols + 4 * count * width * cols,
            transcendentals=0,
        ),
    )(place, *blocks, right, *extra)


def local(design, observations, solution, arc_ids, block_live):
    rows, _ = design.shape
    core, yl, z = lax.axis_index("core"), lax.axis_index("yl"), lax.axis_index("z")
    n = lax.axis_size("z")
    up = [(i, (i + 1) % n) for i in range(n)]
    down = [(i, (i - 1) % n) for i in range(n)]

    gathered = lax.all_gather(design[:, :FIRST], "z", axis=0)
    last = lax.all_gather(design[:, FIRST + WIDTH :], "z", axis=0)

    def start(begin, flip, *tied):
        own = design[:, begin : begin + WIDTH]
        own = after(own, *tied) if tied else own
        return {"ends": [own, own], "blocks": [own], "steps": [0], "flip": flip}

    def hop(ring):
        d = (len(ring["blocks"]) + 1) // 2
        for side in range(2 if d < n // 2 else 1):
            way = up if side == ring["flip"] else down
            end = lax.ppermute(ring["ends"][side], "z", way)
            ring["ends"][side] = end
            ring["blocks"].append(end)
            ring["steps"].append(-d if way is up else d)
        return ring["blocks"][-2:]

    def stacked(ring):
        return lax.rem(z + n + jnp.array(ring["steps"], jnp.int32), n), ring["blocks"]

    early = start(FIRST, 0)
    hops = [hop(early) for _ in range(n // 2)]
    partial_value = jnp.dot(design.astype(f32), solution, precision=lax.Precision.HIGHEST)
    from_pair = lax.ppermute(partial_value, "yl", PAIR)
    other = lax.ppermute(after(design, from_pair), "yl", PAIR)
    predicted = of_everyone(partial_value + from_pair, "z")
    residual = after(observations - predicted, *hops[0])
    live_row = (
        jnp.broadcast_to(block_live[0][:, None], (block_live.shape[1], 128))
        .reshape(rows)
        .astype(f32)
    )
    arc_match = (arc_ids[0][None, :] == jnp.arange(ARCS_DEV, dtype=jnp.int32)[:, None]).astype(f32)
    squares = live_row * residual * residual
    arc_squares = jnp.sum(arc_match * squares[None, :], axis=1)
    arc_counts = jnp.sum(arc_match * live_row[None, :], axis=1)
    totals = of_everyone(jnp.stack([jnp.sum(arc_squares), jnp.sum(arc_counts)]), ARCS)
    variance_all = (totals[0] + 1.0) / (totals[1] + 1.0)
    arc_weight = variance_all / (
        (arc_squares + prior_rows * variance_all) / (arc_counts + prior_rows)
    )
    arc_weight = after(arc_weight, *hops[1])
    row_weight = live_row * jnp.sum(arc_match * arc_weight[:, None], axis=0)
    rhs_part = lax.dot_general(
        design.astype(f32),
        row_weight * residual,
        (((0,), (0,)), ((), ())),
        precision=lax.Precision.HIGHEST,
    )
    rhs_pair = rhs_part + lax.ppermute(rhs_part, "core", PAIR)
    rhs = of_everyone(rhs_pair, ("x", "yh"))
    weighted_own = (row_weight[:, None] * design).astype(bf16)
    weighted_other = (row_weight[:, None] * other).astype(bf16)
    mine = jnp.where(core == yl, weighted_own, weighted_other)
    theirs = jnp.where(core == yl, weighted_other, weighted_own)

    def share(left, right, added=None):
        if isinstance(left, tuple):
            return product(*left, right, added)
        out = lax.dot_general(left, right, (((1,), (0,)), ((), ())), preferred_element_type=f32)
        return out if added is None else (out + added).astype(bf16)

    def spread(pair):
        got = lax.all_to_all(pair, ("x", "yh"), 0, 0, tiled=True)
        block = jnp.sum(got.astype(f32), axis=0)
        return lax.ppermute(block, ("core", "yl"), [(0, 0), (1, 2), (2, 1), (3, 3)])

    def whole_chunk(left, *tied):
        sent = share(left, after(theirs, *tied) if tied else theirs)
        from_core = lax.ppermute(sent, "core", PAIR)
        return share(left, mine, from_core)

    pair_r = whole_chunk(stacked(early))
    hopped = spread(pair_r)
    pair_a = whole_chunk(gathered, pair_r)
    first = spread(pair_a)
    done = [first, hopped, spread(whole_chunk(last))]
    return jnp.concatenate(done, axis=0), rhs


def solution(mesh):
    finer = Mesh(mesh.devices.reshape(4, 2, 2, 8, 2), ARCS + TILES)
    return jax.shard_map(
        local,
        mesh=finer,
        in_specs=(P(ARCS, TILES), P(ARCS), P(TILES), P(ARCS, None), P(ARCS, None)),
        out_specs=(P(ARCS, TILES), P(TILES)),
        check_vma=False,
    )
```

```python
import jax
import jax.numpy as jnp
from jax import lax
from jax.experimental import pallas as pl
from jax.experimental.pallas import tpu as pltpu
from jax.sharding import Mesh
from jax.sharding import PartitionSpec as P

ARCS_DEV = 4
ARCS = ("x", "yh", "core")
TILES = ("z", "yl")
FIRST, WIDTH = 256, 128
prior_rows = 4.0
f32, bf16 = jnp.float32, jnp.bfloat16
PAIR = [(0, 1), (1, 0)]


def after(array, *first):
    return lax.optimization_barrier((array, *first))[0]


def of_everyone(array, axis):
    count = lax.axis_size(axis)
    sent = jnp.broadcast_to(array[None], (count, *array.shape))
    return lax.all_to_all(sent, axis, 0, 0, tiled=True).sum(axis=0)


def product(place, blocks, right):
    count, (rows, width), cols = len(blocks) - 1, blocks[0].shape, right.shape[1]

    def kernel(place_ref, *refs):
        right_ref, out_ref = refs[-2:]
        by_rows = (((0,), (0,)), ((), ()))

        def part(left_ref, begin):
            some = right_ref[begin : begin + left_ref.shape[0]]
            return lax.dot_general(left_ref[...], some, by_rows, preferred_element_type=f32)

        for i in range(count - 1):
            out_ref[place_ref[i]] = part(refs[i], 0)
        out_ref[place_ref[count - 1]] = part(refs[count - 1], 0) + part(refs[count], rows // 2)

    vmem = pl.BlockSpec(memory_space=pltpu.VMEM)
    return pl.pallas_call(
        kernel,
        out_shape=jax.ShapeDtypeStruct((count, width, cols), f32),
        in_specs=[pl.BlockSpec(memory_space=pltpu.SMEM)] + [vmem] * (count + 2),
        out_specs=vmem,
        cost_estimate=pl.CostEstimate(
            flops=2 * count * rows * width * cols,
            bytes_accessed=2 * count * rows * width + 2 * rows * cols + 4 * count * width * cols,
            transcendentals=0,
        ),
    )(place, *blocks, right)


def local(design, observations, solution, arc_ids, block_live):
    rows, _ = design.shape
    core, yl, z = lax.axis_index("core"), lax.axis_index("yl"), lax.axis_index("z")
    n = lax.axis_size("z")
    up = [(i, (i + 1) % n) for i in range(n)]
    down = [(i, (i - 1) % n) for i in range(n)]

    gathered = lax.all_gather(design[:, :FIRST], "z", axis=0)
    last = lax.all_gather(design[:, FIRST + WIDTH :], "z", axis=0)

    def start(begin, flip, *tied):
        own = design[:, begin : begin + WIDTH]
        own = after(own, *tied) if tied else own
        return {"ends": [own, own], "blocks": [own], "steps": [0], "flip": flip}

    def hop(ring):
        d = (len(ring["blocks"]) + 1) // 2
        half = rows // 2
        for side in range(2):
            way = up if side == ring["flip"] else down
            end = ring["ends"][side]
            if d == n // 2:
                end = end[side * half : (side + 1) * half]
            end = lax.ppermute(end, "z", way)
            ring["ends"][side] = end
            ring["blocks"].append(end)
            if d < n // 2 or side == 0:
                ring["steps"].append(-d if way is up else d)
        return ring["blocks"][-2:]

    def stacked(ring):
        return lax.rem(z + n + jnp.array(ring["steps"], jnp.int32), n), ring["blocks"]

    early = start(FIRST, 0)
    hops = [hop(early) for _ in range(n // 2)]
    partial_value = jnp.dot(design.astype(f32), solution, precision=lax.Precision.HIGHEST)
    from_pair = lax.ppermute(partial_value, "yl", PAIR)
    predicted = of_everyone(partial_value + from_pair, "z")
    residual = after(observations - predicted, *hops[0])
    live_row = (
        jnp.broadcast_to(block_live[0][:, None], (block_live.shape[1], 128))
        .reshape(rows)
        .astype(f32)
    )
    arc_match = (arc_ids[0][None, :] == jnp.arange(ARCS_DEV, dtype=jnp.int32)[:, None]).astype(f32)
    squares = live_row * residual * residual
    arc_squares = jnp.sum(arc_match * squares[None, :], axis=1)
    arc_counts = jnp.sum(arc_match * live_row[None, :], axis=1)
    totals = of_everyone(jnp.stack([jnp.sum(arc_squares), jnp.sum(arc_counts)]), ARCS)
    other = lax.ppermute(after(design, totals), "yl", PAIR)
    variance_all = (totals[0] + 1.0) / (totals[1] + 1.0)
    arc_weight = variance_all / (
        (arc_squares + prior_rows * variance_all) / (arc_counts + prior_rows)
    )
    arc_weight = after(arc_weight, *hops[1])
    row_weight = live_row * jnp.sum(arc_match * arc_weight[:, None], axis=0)
    rhs_part = lax.dot_general(
        design.astype(f32),
        row_weight * residual,
        (((0,), (0,)), ((), ())),
        precision=lax.Precision.HIGHEST,
    )
    rhs_pair = rhs_part + lax.ppermute(rhs_part, "core", PAIR)
    rhs = of_everyone(rhs_pair, ("x", "yh"))
    weighted_own = (row_weight[:, None] * design).astype(bf16)
    weighted_other = (row_weight[:, None] * other).astype(bf16)
    mine = jnp.where(core == yl, weighted_own, weighted_other)
    theirs = jnp.where(core == yl, weighted_other, weighted_own)

    def share(left, right, added=None):
        if isinstance(left, tuple):
            out = product(*left, right)
        else:
            out = lax.dot_general(left, right, (((1,), (0,)), ((), ())), preferred_element_type=f32)
        return out if added is None else (out + added).astype(bf16)

    def spread(pair):
        got = lax.all_to_all(pair, ("x", "yh"), 0, 0, tiled=True)
        block = jnp.sum(got.astype(f32), axis=0)
        return lax.ppermute(block, ("core", "yl"), [(0, 0), (1, 2), (2, 1), (3, 3)])

    def whole_chunk(left, *tied):
        sent = share(left, after(theirs, *tied) if tied else theirs)
        from_core = lax.ppermute(sent, "core", PAIR)
        return share(left, mine, from_core)

    pair_r = whole_chunk(stacked(early))
    hopped = spread(pair_r)
    pair_a = whole_chunk(gathered, pair_r)
    first = spread(pair_a)
    done = [first, hopped, spread(whole_chunk(last))]
    return jnp.concatenate(done, axis=0), rhs


def solution(mesh):
    finer = Mesh(mesh.devices.reshape(4, 2, 2, 8, 2), ARCS + TILES)
    return jax.shard_map(
        local,
        mesh=finer,
        in_specs=(P(ARCS, TILES), P(ARCS), P(TILES), P(ARCS, None), P(ARCS, None)),
        out_specs=(P(ARCS, TILES), P(TILES)),
        check_vma=False,
    )
```

```python
import jax
import jax.numpy as jnp
from jax import lax
from jax.experimental import pallas as pl
from jax.experimental.layout import Layout, with_layout_constraint
from jax.experimental.pallas import tpu as pltpu
from jax.sharding import Mesh
from jax.sharding import PartitionSpec as P

ARCS_DEV = 4
ARCS = ("x", "yh", "core")
TILES = ("z", "yl")
FIRST, WIDTH = 256, 128
prior_rows = 4.0
f32, bf16 = jnp.float32, jnp.bfloat16
PAIR = [(0, 1), (1, 0)]


def after(array, *first):
    return lax.optimization_barrier((array, *first))[0]


def of_everyone(array, axis):
    count = lax.axis_size(axis)
    sent = jnp.broadcast_to(array[None], (count, *array.shape))
    return lax.all_to_all(sent, axis, 0, 0, tiled=True).sum(axis=0)


def product(place, blocks, right):
    count, (rows, width), cols = len(blocks) - 1, blocks[0].shape, right.shape[1]

    def kernel(place_ref, *refs):
        right_ref, out_ref = refs[-2:]
        by_rows = (((0,), (0,)), ((), ()))

        def part(left_ref, begin):
            some = right_ref[begin : begin + left_ref.shape[0]]
            return lax.dot_general(left_ref[...], some, by_rows, preferred_element_type=f32)

        for i in range(count - 1):
            out_ref[place_ref[i]] = part(refs[i], 0)
        out_ref[place_ref[count - 1]] = part(refs[count - 1], 0) + part(refs[count], rows // 2)

    vmem = pl.BlockSpec(memory_space=pltpu.VMEM)
    return pl.pallas_call(
        kernel,
        out_shape=jax.ShapeDtypeStruct((count, width, cols), f32),
        in_specs=[pl.BlockSpec(memory_space=pltpu.SMEM)] + [vmem] * (count + 2),
        out_specs=vmem,
        cost_estimate=pl.CostEstimate(
            flops=2 * count * rows * width * cols,
            bytes_accessed=2 * count * rows * width + 2 * rows * cols + 4 * count * width * cols,
            transcendentals=0,
        ),
    )(place, *blocks, right)


def local(design, observations, solution, arc_ids, block_live):
    rows, _ = design.shape
    core, yl, z = lax.axis_index("core"), lax.axis_index("yl"), lax.axis_index("z")
    n = lax.axis_size("z")
    up = [(i, (i + 1) % n) for i in range(n)]
    down = [(i, (i - 1) % n) for i in range(n)]

    gathered = lax.all_gather(design[:, :FIRST], "z", axis=0)
    last = lax.all_gather(design[:, FIRST + WIDTH :], "z", axis=0)

    def start(begin, flip, *tied):
        own = design[:, begin : begin + WIDTH]
        own = after(own, *tied) if tied else own
        return {"ends": [own, own], "blocks": [own], "steps": [0], "flip": flip}

    def hop(ring):
        d = (len(ring["blocks"]) + 1) // 2
        half = rows // 2
        for side in range(2):
            way = up if side == ring["flip"] else down
            end = ring["ends"][side]
            if d == n // 2:
                end = end[side * half : (side + 1) * half]
            end = lax.ppermute(end, "z", way)
            ring["ends"][side] = end
            ring["blocks"].append(end)
            if d < n // 2 or side == 0:
                ring["steps"].append(-d if way is up else d)
        return ring["blocks"][-2:]

    def stacked(ring):
        return lax.rem(z + n + jnp.array(ring["steps"], jnp.int32), n), ring["blocks"]

    early = start(FIRST, 0)
    hops = [hop(early) for _ in range(n // 2)]
    partial_value = jnp.dot(design.astype(f32), solution, precision=lax.Precision.HIGHEST)
    from_pair = lax.ppermute(partial_value, "yl", PAIR)
    predicted = of_everyone(partial_value + from_pair, "z")
    residual = after(observations - predicted, *hops[0])
    live_row = (
        jnp.broadcast_to(block_live[0][:, None], (block_live.shape[1], 128))
        .reshape(rows)
        .astype(f32)
    )
    arc_match = (arc_ids[0][None, :] == jnp.arange(ARCS_DEV, dtype=jnp.int32)[:, None]).astype(f32)
    squares = live_row * residual * residual
    arc_squares = jnp.sum(arc_match * squares[None, :], axis=1)
    arc_counts = jnp.sum(arc_match * live_row[None, :], axis=1)
    totals = of_everyone(jnp.stack([jnp.sum(arc_squares), jnp.sum(arc_counts)]), ARCS)
    other = lax.ppermute(after(design, totals), "yl", PAIR)
    variance_all = (totals[0] + 1.0) / (totals[1] + 1.0)
    arc_weight = variance_all / (
        (arc_squares + prior_rows * variance_all) / (arc_counts + prior_rows)
    )
    arc_weight = after(arc_weight, *hops[1])
    row_weight = live_row * jnp.sum(arc_match * arc_weight[:, None], axis=0)
    rhs_part = lax.dot_general(
        design.astype(f32),
        row_weight * residual,
        (((0,), (0,)), ((), ())),
        precision=lax.Precision.HIGHEST,
    )
    rhs_pair = rhs_part + lax.ppermute(rhs_part, "core", PAIR)
    rhs = of_everyone(rhs_pair, ("x", "yh"))
    weighted_own = (row_weight[:, None] * design).astype(bf16)
    weighted_other = (row_weight[:, None] * other).astype(bf16)
    mine = jnp.where(core == yl, weighted_own, weighted_other)
    theirs = jnp.where(core == yl, weighted_other, weighted_own)

    def share(left, right, added=None):
        if isinstance(left, tuple):
            out = product(*left, right)
        else:
            out = lax.dot_general(left, right, (((1,), (0,)), ((), ())), preferred_element_type=f32)
        if added is None:
            return out
        return (lax.optimization_barrier(out) + added).astype(bf16)

    def spread(pair):
        got = lax.all_to_all(pair, ("x", "yh"), 0, 0, tiled=True)
        block = jnp.sum(got.astype(f32), axis=0)
        block = with_layout_constraint(block, Layout((0, 1)))
        return lax.ppermute(block, ("core", "yl"), [(0, 0), (1, 2), (2, 1), (3, 3)])

    def whole_chunk(left, *tied):
        sent = share(left, after(theirs, *tied) if tied else theirs)
        from_core = lax.ppermute(sent, "core", PAIR)
        return share(left, mine, from_core)

    pair_r = whole_chunk(stacked(early))
    hopped = spread(pair_r)
    pair_a = whole_chunk(gathered, pair_r)
    first = spread(pair_a)
    done = [first, hopped, spread(whole_chunk(last))]
    return jnp.concatenate(done, axis=0), rhs


def solution(mesh):
    finer = Mesh(mesh.devices.reshape(4, 2, 2, 8, 2), ARCS + TILES)
    return jax.shard_map(
        local,
        mesh=finer,
        in_specs=(P(ARCS, TILES), P(ARCS), P(TILES), P(ARCS, None), P(ARCS, None)),
        out_specs=(P(ARCS, TILES), P(TILES)),
        check_vma=False,
    )
```
